32 devices in a mesh: seq: 8 (over z, y), tp: 4 (over x, core).
Axes of the slice: x: 2, y: 2, z: 4, core: 2. Of those that a mesh axis runs over, the one named last changes fastest.
Arguments:
- tokens: bfloat16 [4096, 2560], P('seq', 'tp'), may hold values from -6 to 6
- gate_weight: bfloat16 [2560, 5120], P(None, 'tp'), may hold values from -0.125 to 0.125
- inner_weight: bfloat16 [2560, 5120], P(None, 'tp'), may hold values from -0.125 to 0.125
- state_weight: bfloat16 [2560, 256], replicated, may hold values from -0.125 to 0.125
- step_weight: bfloat16 [2560, 80], P(None, 'tp'), may hold values from -0.125 to 0.125
- conv_inner: float32 [4, 5120], P(None, 'tp'), may hold values from -3 to 3
- conv_state: float32 [4, 256], replicated, may hold values from -3 to 3
- step_bias: float32 [80], P('tp'), may hold values from -3 to 1
- decay_rate: float32 [80], P('tp'), may hold values from 1e-05 to 0.02
- skip_gain: float32 [80], P('tp'), may hold values from 0.5 to 2
- norm_gain: float32 [5120], P('tp'), may hold values from 0.1 to 1.9
- out_weight: bfloat16 [5120, 2560], P('tp'), may hold values from -0.078125 to 0.078125
Outputs:
- layer_out: bfloat16 [4096, 2560], P(('seq', 'tp'))
The draws below stay inside these ranges and needn't reach their ends.
All inputs are finite; a program needn't handle non-finite values.
Results may differ from the reference program's by a relative error of at most 0.018.
Values may be sent and summed in bfloat16 or wider, within the bound.
A program may use at most 128 MiB of HBM per device.

```python
import math
import jax
import jax.numpy as jnp
from jax import lax

D = 2560
HEADS = 80
HEAD_DIM = 64
STATE = 128
KERNEL = 4
GROUP = 256
INNER = 5120
TOKENS = 4096


def block_levels(stream_key, shape, shards, smallest, top_value):
    def one(position, parts):
        steps = jax.random.uniform(jax.random.fold_in(jax.random.fold_in(stream_key, 6), position), (parts,), jnp.float32, smallest / len(shards), top_value / len(shards))
        return jnp.repeat(jnp.exp(steps), shape[position] // parts).reshape((-1,) + (1,) * (len(shape) - position - 1))

    level = one(*shards[0])
    for cut in shards[1:]:
        level = level * one(*cut)
    return level


def centred(rng, shape, width, reach, split=(), kind=jnp.bfloat16):
    array = width * jax.random.normal(rng, shape, jnp.float32)
    if split:
        array = array * block_levels(rng, shape, split, -0.22, 0.18)
    return jnp.clip(array, -reach, reach).astype(kind)


def setup_inputs(seed: int = 0) -> dict:
    key_list = jax.random.split(jax.random.key(seed), 13)
    return {
        "tokens": centred(key_list[0], (TOKENS, D), 1.0, 6.0, ((0, 8), (1, 4))),
        "gate_weight": centred(key_list[1], (D, INNER), D ** -0.5, 0.125, ((1, 4),)),
        "inner_weight": centred(key_list[2], (D, INNER), D ** -0.5, 0.125, ((1, 4),)),
        "state_weight": centred(key_list[3], (D, 2 * STATE), D ** -0.5, 0.125),
        "step_weight": centred(key_list[4], (D, HEADS), D ** -0.5, 0.125, ((1, 4),)),
        "conv_inner": centred(key_list[5], (KERNEL, INNER), KERNEL ** -0.5, 3.0, ((1, 4),), jnp.float32),
        "conv_state": centred(key_list[6], (KERNEL, 2 * STATE), KERNEL ** -0.5, 3.0, (), jnp.float32),
        "step_bias": jnp.clip(-3.0 + 4.0 * jax.random.uniform(key_list[7], (HEADS,), jnp.float32) ** block_levels(key_list[7], (HEADS,), ((0, 4),), -0.2, 0.2), -3.0, 1.0),
        "decay_rate": jnp.clip(jnp.exp(math.log(0.02) - 7.6009025 * jax.random.uniform(key_list[8], (HEADS,), jnp.float32) ** block_levels(key_list[8], (HEADS,), ((0, 4),), -0.2, 0.2)), 9.999999747378752e-06, 0.02),
        "skip_gain": jnp.clip(0.5 + 1.5 * jax.random.uniform(key_list[9], (HEADS,), jnp.float32) ** block_levels(key_list[9], (HEADS,), ((0, 4),), -0.2, 0.2), 0.5, 2.0),
        "norm_gain": jnp.clip(1.0 + 0.18 * jax.random.normal(key_list[10], (INNER,), jnp.float32), 0.1, 1.9),
        "out_weight": centred(key_list[11], (INNER, D), INNER ** -0.5, 0.078125, ((0, 4),)),
    }


def reference(tokens, gate_weight, inner_weight, state_weight, step_weight, conv_inner, conv_state, step_bias, decay_rate, skip_gain, norm_gain, out_weight):
    gate_act = jnp.dot(tokens, gate_weight, preferred_element_type=jnp.float32).astype(jnp.bfloat16)
    mixed_in = jnp.concatenate([jnp.dot(tokens, inner_weight, preferred_element_type=jnp.float32), jnp.dot(tokens, state_weight, preferred_element_type=jnp.float32)], axis=1).astype(jnp.bfloat16)
    step_raw = jnp.dot(tokens, step_weight, preferred_element_type=jnp.float32)
    kernel = jnp.concatenate([conv_inner, conv_state], axis=1)
    padded = jnp.concatenate([jnp.zeros((KERNEL - 1, mixed_in.shape[1]), jnp.bfloat16), mixed_in], axis=0)
    conv_sum = jnp.zeros(mixed_in.shape, jnp.float32)
    for tap in range(KERNEL):
        conv_sum = conv_sum + padded[tap:tap + TOKENS].astype(jnp.float32) * kernel[tap][None, :]
    conv_out = jax.nn.silu(conv_sum).astype(jnp.bfloat16)
    inner_act = conv_out[:, :INNER].reshape(TOKENS, HEADS, HEAD_DIM)
    inject = conv_out[:, INNER:INNER + STATE]
    readout = conv_out[:, INNER + STATE:]
    time_step = jax.nn.softplus(step_raw + step_bias[None, :])
    log_decay = -time_step * decay_rate[None, :]
    blocks = TOKENS // GROUP
    causal = jnp.arange(GROUP)[:, None] >= jnp.arange(GROUP)[None, :]
    highest = lax.Precision.HIGHEST

    def advance(carried, block):
        inner_blk, inject_blk, readout_blk, step_blk, log_blk = block
        cumulative = jnp.cumsum(log_blk, axis=0)
        scores = jnp.dot(readout_blk, inject_blk.T, preferred_element_type=jnp.float32)
        log_gaps = cumulative.T[:, :, None] - cumulative.T[:, None, :]
        decay_mask = jnp.exp(jnp.where(causal[None], log_gaps, -jnp.inf))
        mixing = (scores[None] * decay_mask * step_blk.T[:, None, :]).astype(jnp.bfloat16)
        intra_out = jnp.einsum('hts,shp->thp', mixing.astype(jnp.float32), inner_blk.astype(jnp.float32), precision=highest)
        state_reads = jnp.einsum('tn,hpn->thp', readout_blk.astype(jnp.float32), carried, precision=highest) * jnp.exp(cumulative)[:, :, None]
        ending = cumulative[-1]
        tail_weight = jnp.exp(ending[None, :] - cumulative) * step_blk
        contribution = jnp.einsum('thp,tn->hpn', inner_blk.astype(jnp.float32) * tail_weight[:, :, None], inject_blk.astype(jnp.float32), precision=highest)
        carried = jnp.exp(ending)[:, None, None] * carried + contribution
        return (carried, intra_out + state_reads)
    start_state = jnp.zeros((HEADS, HEAD_DIM, STATE), jnp.float32)
    stacked = (inner_act.reshape(blocks, GROUP, HEADS, HEAD_DIM), inject.reshape(blocks, GROUP, STATE), readout.reshape(blocks, GROUP, STATE), time_step.reshape(blocks, GROUP, HEADS), log_decay.reshape(blocks, GROUP, HEADS))
    final_state, block_outs = lax.scan(advance, start_state, stacked)
    ssd_out = block_outs.reshape(TOKENS, HEADS, HEAD_DIM) + skip_gain[None, :, None] * inner_act.astype(jnp.float32)
    gated = ssd_out.reshape(TOKENS, INNER) * jax.nn.silu(gate_act.astype(jnp.float32))
    mean_square = lax.optimization_barrier(jnp.mean(gated * gated, axis=1))
    normed = (gated * lax.rsqrt(mean_square + 1e-05)[:, None] * norm_gain[None, :]).astype(jnp.bfloat16)
    return jnp.dot(normed, out_weight, preferred_element_type=jnp.float32).astype(jnp.bfloat16)
```

```python
import jax
import jax.numpy as jnp
from jax import lax
from jax.sharding import PartitionSpec as P

GROUP = 256
HALO = 16


def swapped(shard, by):
    size = lax.axis_size("tp")
    return lax.ppermute(shard, "tp", [(i, i ^ by) for i in range(size)])


def shifted(shard, by):
    size = lax.axis_size("seq")
    return lax.ppermute(shard, "seq", [(i, i + by) for i in range(size - by)])


def gather_features(rows):
    size = lax.axis_size("tp")
    me = lax.axis_index("tp")
    width = rows.shape[1]
    held = [(0, rows)]
    step = size // 2
    while step >= 1:
        held = held + [(code ^ step, swapped(part, step)) for code, part in held]
        step //= 2
    parts = dict(held)
    full = jnp.zeros((rows.shape[0], width * size), rows.dtype)
    for code in range(size):
        full = lax.dynamic_update_slice(full, parts[code], (0, (me ^ code) * width))
    return full


def sum_over_tp(part):
    size = lax.axis_size("tp")
    step = 1
    while step < size:
        part = part + swapped(part, step)
        step *= 2
    return part


def earlier_state(local_state, decay_total):
    size = lax.axis_size("seq")
    heads, width, states = local_state.shape
    rows = heads * width
    me = lax.axis_index("seq")
    decay_all = lax.all_gather(decay_total[None, :], "seq", axis=0, tiled=True)
    row_decay = jnp.exp(jnp.repeat(decay_all, width, axis=1))
    row_decay = lax.dynamic_slice(row_decay, (0, me * (rows // size)), (size, rows // size))
    blocks = local_state.astype(jnp.bfloat16).reshape(size, rows // size, states)
    mine = lax.all_to_all(blocks, "seq", 0, 0, tiled=True)
    carried = jnp.zeros((rows // size, states), jnp.float32)
    prefixes = []
    for i in range(size):
        prefixes.append(carried.astype(jnp.bfloat16))
        carried = carried * row_decay[i][:, None] + mine[i].astype(jnp.float32)
    back = lax.all_to_all(jnp.stack(prefixes), "seq", 0, 0, tiled=True)
    return back.reshape(heads, width, states)


def project(rows, *weights):
    return [jnp.dot(rows, weight, preferred_element_type=jnp.float32) for weight in weights]


def convolve(padded, kernel, length):
    taps = kernel.shape[0]
    start = padded.shape[0] - length - (taps - 1)
    total = jnp.zeros((length, padded.shape[1]), jnp.float32)
    for tap in range(taps):
        total = total + padded[start + tap : start + tap + length].astype(jnp.float32) * kernel[tap][None, :]
    return jax.nn.silu(total).astype(jnp.bfloat16)


def on_device(
    tokens,
    gate_weight,
    inner_weight,
    state_weight,
    step_weight,
    conv_inner,
    conv_state,
    step_bias,
    decay_rate,
    skip_gain,
    norm_gain,
    out_weight,
):
    tok_rows = tokens.shape[0]
    width_inner = inner_weight.shape[1]
    head_count = step_weight.shape[1]
    head_width = width_inner // head_count
    state_size = state_weight.shape[1] // 2
    blocks = tok_rows // GROUP
    size_tp = lax.axis_size("tp")
    me = lax.axis_index("tp")

    halo = shifted(tokens[tok_rows - HALO :], 1)
    chunks = [None] * blocks
    for b in range(blocks - 1, -1, -1):
        rows = tokens[b * GROUP : (b + 1) * GROUP]
        if b == 0:
            rows = jnp.concatenate([halo, rows], axis=0)
        chunks[b] = gather_features(rows)

    inner_raw, state_raw, step_raw = [None] * blocks, [None] * blocks, [None] * blocks
    for b in range(blocks - 1, -1, -1):
        i_b, s_b, t_b = project(chunks[b], inner_weight, state_weight, step_weight)
        inner_raw[b], state_raw[b] = i_b.astype(jnp.bfloat16), s_b.astype(jnp.bfloat16)
        step_raw[b] = t_b[HALO:] if b == 0 else t_b

    local_state = jnp.zeros((head_count, head_width, state_size), jnp.float32)
    decay_total = jnp.zeros((head_count,), jnp.float32)
    pieces = []
    for b in range(blocks):
        if b == 0:
            pad_i, pad_s = inner_raw[0], state_raw[0]
        else:
            pad_i = jnp.concatenate([inner_raw[b - 1][-HALO:], inner_raw[b]], axis=0)
            pad_s = jnp.concatenate([state_raw[b - 1][-HALO:], state_raw[b]], axis=0)
        x = convolve(pad_i, conv_inner, GROUP)
        bc = convolve(pad_s, conv_state, GROUP)
        inject, readout = bc[:, :state_size], bc[:, state_size:]
        time_step = jax.nn.softplus(step_raw[b] + step_bias[None, :])
        log_decay = -time_step * decay_rate[None, :]
        cumulative = jnp.cumsum(log_decay, axis=0)
        ending = cumulative[-1]
        tail = jnp.exp(ending[None, :] - cumulative) * time_step
        scaled = (x.astype(jnp.float32) * jnp.repeat(tail, head_width, axis=1)).astype(jnp.bfloat16)
        contribution = lax.dot_general(
            scaled, inject, (((0,), (0,)), ((), ())), preferred_element_type=jnp.float32
        ).reshape(head_count, head_width, state_size)
        local_state = jnp.exp(ending)[:, None, None] * local_state + contribution
        decay_total = decay_total + ending
        pieces.append((x, inject, readout, time_step, cumulative, ending, contribution))

    carried = earlier_state(local_state, decay_total).astype(jnp.float32)

    gated, squares = [], []
    for b in range(blocks):
        x, inject, readout, time_step, cumulative, ending, contribution = pieces[b]
        gate_rows = chunks[b][HALO:] if b == 0 else chunks[b]
        gate = jnp.dot(gate_rows, gate_weight, preferred_element_type=jnp.float32).astype(jnp.bfloat16)
        scores = lax.dot_general(
            readout, inject, (((1,), (1,)), ((), ())), preferred_element_type=jnp.float32
        )
        causal = jnp.arange(GROUP)[:, None] >= jnp.arange(GROUP)[None, :]
        gaps = cumulative.T[:, :, None] - cumulative.T[:, None, :]
        mask = jnp.exp(jnp.where(causal[None], gaps, -jnp.inf))
        mixing = (scores[None] * mask * time_step.T[:, None, :]).astype(jnp.bfloat16)
        x3 = x.reshape(GROUP, head_count, head_width)
        intra = jnp.einsum("hts,shp->thp", mixing, x3, preferred_element_type=jnp.float32)
        state_b = carried.astype(jnp.bfloat16).reshape(width_inner, state_size)
        reads = lax.dot_general(
            readout, state_b, (((1,), (1,)), ((), ())), preferred_element_type=jnp.float32
        )
        grown = jnp.repeat(jnp.exp(cumulative), head_width, axis=1)
        skip = jnp.repeat(skip_gain, head_width)[None, :]
        ssd = intra.reshape(GROUP, width_inner) + reads * grown + skip * x.astype(jnp.float32)
        g = ssd * jax.nn.silu(gate.astype(jnp.float32))
        squares.append(jnp.sum(g * g, axis=1))
        gated.append((g * norm_gain[None, :]).astype(jnp.bfloat16))
        carried = jnp.exp(ending)[:, None, None] * carried + contribution

    gated = jnp.concatenate(gated, axis=0)
    square_total = sum_over_tp(jnp.concatenate(squares, axis=0))
    share = tok_rows // size_tp
    mean_square = lax.dynamic_slice(square_total, (me * share,), (share,)) / (width_inner * size_tp)
    scale = lax.rsqrt(mean_square + 1e-05)[:, None]

    if size_tp != 4:
        part = jnp.dot(gated, out_weight, preferred_element_type=jnp.float32).astype(jnp.bfloat16)
        total = lax.psum_scatter(part, "tp", scatter_dimension=0, tiled=True)
        return (total.astype(jnp.float32) * scale).astype(jnp.bfloat16)

    def rows_of(place):
        return lax.dynamic_slice(gated, (place * share, 0), (share, width_inner))

    def reduced(place, weight):
        away = jnp.dot(rows_of(place ^ 1), weight, preferred_element_type=jnp.float32)
        own = jnp.dot(rows_of(place), weight, preferred_element_type=jnp.float32)
        return own + swapped(away.astype(jnp.bfloat16), 1).astype(jnp.float32)

    cuts = 2
    width_out = out_weight.shape[1] // cuts
    results = []
    weights = [out_weight[:, c * width_out : (c + 1) * width_out] for c in range(cuts)]
    arrived = [swapped(reduced(me ^ 2, w).astype(jnp.bfloat16), 2) for w in weights]
    for w, other in zip(weights, arrived):
        total = reduced(me, w) + other.astype(jnp.float32)
        results.append((total * scale).astype(jnp.bfloat16))
    return jnp.concatenate(results, axis=1)


def solution(mesh):
    in_specs = (
        P("seq", "tp"),
        P(None, "tp"),
        P(None, "tp"),
        P(),
        P(None, "tp"),
        P(None, "tp"),
        P(),
        P("tp"),
        P("tp"),
        P("tp"),
        P("tp"),
        P("tp", None),
    )
    out_specs = P(("seq", "tp"), None)
    return jax.shard_map(
        on_device, mesh=mesh, in_specs=in_specs, out_specs=out_specs, check_vma=False
    )
```

```python
import jax
import jax.numpy as jnp
from jax import lax
from jax.experimental import pallas as pl
from jax.experimental.pallas import tpu as pltpu
from jax.sharding import PartitionSpec as P

GROUP = 256
HALO = 16


def swapped(shard, by):
    size = lax.axis_size("tp")
    return lax.ppermute(shard, "tp", [(i, i ^ by) for i in range(size)])


def shifted(shard, by):
    size = lax.axis_size("seq")
    return lax.ppermute(shard, "seq", [(i, i + by) for i in range(size - by)])


def gather_features(rows):
    size = lax.axis_size("tp")
    me = lax.axis_index("tp")
    width = rows.shape[1]
    held = [(0, rows)]
    step = size // 2
    while step >= 1:
        held = held + [(code ^ step, swapped(part, step)) for code, part in held]
        step //= 2
    parts = dict(held)
    full = jnp.zeros((rows.shape[0], width * size), rows.dtype)
    for code in range(size):
        full = lax.dynamic_update_slice(full, parts[code], (0, (me ^ code) * width))
    return full


def sum_over_tp(part):
    size = lax.axis_size("tp")
    step = 1
    while step < size:
        part = part + swapped(part, step)
        step *= 2
    return part


def prefix_kernel(mine_ref, decay_ref, owner_ref, out_ref):
    owner = owner_ref[...]
    carried = jnp.zeros(mine_ref.shape[1:], jnp.float32)
    for i in range(mine_ref.shape[0]):
        out_ref[i] = carried.astype(jnp.bfloat16)
        log_row = jnp.sum(owner * decay_ref[i : i + 1, :], axis=1, keepdims=True)
        carried = carried * jnp.exp(log_row) + mine_ref[i].astype(jnp.float32)


def earlier_state(local_state, decay_total, head_width):
    size = lax.axis_size("seq")
    rows, states = local_state.shape
    share = rows // size
    me = lax.axis_index("seq")
    decay_all = lax.all_gather(decay_total[None, :], "seq", axis=0, tiled=True)
    blocks = local_state.reshape(size, share, states)
    blocks, decay_all = lax.optimization_barrier((blocks, decay_all))
    mine = lax.all_to_all(blocks, "seq", 0, 0, tiled=True)
    row_head = (me * share + jnp.arange(share)) // head_width
    owner = (row_head[:, None] == jnp.arange(decay_total.shape[0])[None, :]).astype(jnp.float32)
    prefixes = pl.pallas_call(
        prefix_kernel,
        out_shape=jax.ShapeDtypeStruct(mine.shape, jnp.bfloat16),
        cost_estimate=pl.CostEstimate(flops=0, bytes_accessed=4 * mine.size, transcendentals=0),
    )(mine, decay_all, owner)
    return lax.all_to_all(prefixes, "seq", 0, 0, tiled=True).reshape(rows, states)


def per_head(table, first, count, width, lanes):
    lane = lax.broadcasted_iota(jnp.int32, (table.shape[0], lanes), 1)
    spread = jnp.broadcast_to(table[:, first : first + 1], (table.shape[0], lanes))
    for k in range(1, count):
        spread = jnp.where(lane >= k * width, table[:, first + k : first + k + 1], spread)
    return spread


def silu(value):
    return value * (0.5 * jnp.tanh(0.5 * value) + 0.5)


def conv_kernel(blocks, head_width, lanes, *refs):
    inner_refs, state_refs = refs[:blocks], refs[blocks : 2 * blocks]
    tap_inner, tap_state, tail_ref = refs[2 * blocks : 2 * blocks + 3]
    x_ref, bc_ref, contribution_ref = refs[2 * blocks + 3 :]
    taps = tap_inner.shape[0]
    heads_per = lanes // head_width

    def mixed(chunk_refs, b, span, kernel):
        if b == 0:
            padded = chunk_refs[0][:, span].astype(jnp.float32)
        else:
            last = chunk_refs[b - 1].shape[0] - HALO
            edge = chunk_refs[b - 1][last:, span].astype(jnp.float32)
            padded = jnp.concatenate([edge, chunk_refs[b][:, span].astype(jnp.float32)], axis=0)
        total = padded * kernel[taps - 1 : taps]
        for tap in range(taps - 1):
            total = total + pltpu.roll(padded, taps - 1 - tap, 0) * kernel[tap : tap + 1]
        return silu(total[HALO:]).astype(jnp.bfloat16)

    for b in range(blocks):
        rows = slice(b * GROUP, (b + 1) * GROUP)
        bc = mixed(state_refs, b, slice(None), tap_state[...])
        bc_ref[rows] = bc
        inject = bc[:, : bc.shape[1] // 2]
        tail = tail_ref[rows]
        for p in range(x_ref.shape[1] // lanes):
            span = slice(p * lanes, (p + 1) * lanes)
            x = mixed(inner_refs, b, span, tap_inner[:, span])
            x_ref[rows, span] = x
            weight = per_head(tail, p * heads_per, heads_per, head_width, lanes)
            scaled = (x.astype(jnp.float32) * weight).astype(jnp.bfloat16)
            contribution_ref[b, span] = lax.dot_general(
                scaled, inject, (((0,), (0,)), ((), ())), preferred_element_type=jnp.float32
            )


def intra_kernel(head_width, lanes, x_ref, bc_ref, cum_ref, cum_t_ref, step_t_ref, skip_ref, out_ref):
    states = bc_ref.shape[1] // 2
    heads_per = lanes // head_width
    scores = lax.dot_general(
        bc_ref[:, states:], bc_ref[:, :states], (((1,), (1,)), ((), ())),
        preferred_element_type=jnp.float32,
    )
    t = lax.broadcasted_iota(jnp.int32, scores.shape, 0)
    s = lax.broadcasted_iota(jnp.int32, scores.shape, 1)
    scores = jnp.where(s <= t, scores, 0.0)
    lane = lax.broadcasted_iota(jnp.int32, (x_ref.shape[0], lanes), 1)
    for p in range(x_ref.shape[1] // lanes):
        span = slice(p * lanes, (p + 1) * lanes)
        x = x_ref[:, span]
        total = None
        for k in range(heads_per):
            h = p * heads_per + k
            gaps = jnp.minimum(cum_ref[:, h : h + 1] - cum_t_ref[h : h + 1, :], 0.0)
            mixing = (scores * jnp.exp(gaps) * step_t_ref[h : h + 1, :]).astype(jnp.bfloat16)
            part = jnp.dot(mixing, x, preferred_element_type=jnp.float32)
            total = part if k == 0 else jnp.where(lane >= k * head_width, part, total)
        out_ref[:, span] = total + skip_ref[:, span] * x.astype(jnp.float32)


def gate_kernel(head_width, lanes, intra_ref, bc_ref, cum_ref, gate_ref, gain_ref, state_ref, out_ref, square_ref):
    states = bc_ref.shape[1] // 2
    heads_per = lanes // head_width
    readout = bc_ref[:, states:]
    grown = jnp.exp(cum_ref[...])
    squares = jnp.zeros((readout.shape[0], lanes), jnp.float32)
    for p in range(intra_ref.shape[1] // lanes):
        span = slice(p * lanes, (p + 1) * lanes)
        reads = lax.dot_general(
            readout, state_ref[0, span], (((1,), (1,)), ((), ())), preferred_element_type=jnp.float32
        )
        weight = per_head(grown, p * heads_per, heads_per, head_width, lanes)
        g = (intra_ref[:, span] + reads * weight) * silu(gate_ref[:, span].astype(jnp.float32))
        squares = squares + g * g
        out_ref[:, span] = (g * gain_ref[:, span]).astype(jnp.bfloat16)
    square_ref[...] = jnp.sum(squares, axis=1, keepdims=True)


def project(rows, *weights):
    return [jnp.dot(rows, weight, preferred_element_type=jnp.float32) for weight in weights]


def on_device(
    tokens,
    gate_weight,
    inner_weight,
    state_weight,
    step_weight,
    conv_inner,
    conv_state,
    step_bias,
    decay_rate,
    skip_gain,
    norm_gain,
    out_weight,
):
    tok_rows = tokens.shape[0]
    width_inner = inner_weight.shape[1]
    head_count = step_weight.shape[1]
    head_width = width_inner // head_count
    state_size = state_weight.shape[1] // 2
    blocks = tok_rows // GROUP
    size_tp = lax.axis_size("tp")
    me = lax.axis_index("tp")

    halo = shifted(tokens[tok_rows - HALO :], 1)
    chunks = [None] * blocks
    for b in range(blocks - 1, -1, -1):
        rows = tokens[b * GROUP : (b + 1) * GROUP]
        if b == 0:
            rows = jnp.concatenate([halo, rows], axis=0)
        chunks[b] = gather_features(rows)

    inner_raw, state_raw, step_raw = [None] * blocks, [None] * blocks, [None] * blocks
    for b in range(blocks - 1, -1, -1):
        i_b, s_b, t_b = project(chunks[b], inner_weight, state_weight, step_weight)
        inner_raw[b], state_raw[b] = i_b.astype(jnp.bfloat16), s_b.astype(jnp.bfloat16)
        step_raw[b] = t_b[HALO:] if b == 0 else t_b

    lanes = max(128, head_width)
    time_step = jax.nn.softplus(jnp.concatenate(step_raw, axis=0) + step_bias[None, :])
    log_decay = -time_step * decay_rate[None, :]
    grouped = log_decay.reshape(blocks, GROUP, head_count)
    cumulative = jnp.cumsum(grouped, axis=1)
    ending = cumulative[:, -1]
    tail = (jnp.exp(ending[:, None] - cumulative)).reshape(tok_rows, head_count) * time_step
    cumulative = cumulative.reshape(tok_rows, head_count)

    def cost(flops, count, exps):
        return pl.CostEstimate(flops=flops, bytes_accessed=count, transcendentals=exps)

    whole = tok_rows * width_inner
    x, bc, contribution = pl.pallas_call(
        lambda *refs: conv_kernel(blocks, head_width, lanes, *refs),
        out_shape=(
            jax.ShapeDtypeStruct((tok_rows, width_inner), jnp.bfloat16),
            jax.ShapeDtypeStruct((tok_rows, 2 * state_size), jnp.bfloat16),
            jax.ShapeDtypeStruct((blocks, width_inner, state_size), jnp.float32),
        ),
        cost_estimate=cost(2 * whole * state_size, 6 * whole, whole),
        name="conv",
    )(*inner_raw, *state_raw, conv_inner, conv_state, tail)
    contribution = contribution.reshape(blocks, head_count, head_width, state_size)
    local_state = jnp.zeros((head_count, head_width, state_size), jnp.float32)
    for b in range(blocks):
        local_state = jnp.exp(ending[b])[:, None, None] * local_state + contribution[b]

    def by_rows(width):
        return pl.BlockSpec((GROUP, width), lambda b: (b, 0))

    def by_columns(height):
        return pl.BlockSpec((height, GROUP), lambda b: (0, b))

    def fixed(width):
        return pl.BlockSpec((1, width), lambda b: (0, 0))

    intra = pl.pallas_call(
        lambda *refs: intra_kernel(head_width, lanes, *refs),
        grid=(blocks,),
        in_specs=[
            by_rows(width_inner),
            by_rows(2 * state_size),
            by_rows(head_count),
            by_columns(head_count),
            by_columns(head_count),
            fixed(width_inner),
        ],
        out_specs=by_rows(width_inner),
        out_shape=jax.ShapeDtypeStruct((tok_rows, width_inner), jnp.float32),
        cost_estimate=cost(4 * whole * GROUP, 6 * whole, GROUP * tok_rows * head_count),
        name="intra",
    )(x, bc, cumulative, cumulative.T, time_step.T, jnp.repeat(skip_gain, head_width)[None, :])

    gate = jnp.concatenate(
        [
            jnp.dot(c[c.shape[0] - GROUP :], gate_weight, preferred_element_type=jnp.float32).astype(jnp.bfloat16)
            for c in chunks
        ],
        axis=0,
    )

    carried = earlier_state(
        local_state.astype(jnp.bfloat16).reshape(width_inner, state_size),
        jnp.sum(ending, axis=0),
        head_width,
    ).astype(jnp.float32).reshape(head_count, head_width, state_size)
    states = []
    for b in range(blocks):
        states.append(carried.astype(jnp.bfloat16).reshape(1, width_inner, state_size))
        carried = jnp.exp(ending[b])[:, None, None] * carried + contribution[b]

    gated, squares = pl.pallas_call(
        lambda *refs: gate_kernel(head_width, lanes, *refs),
        grid=(blocks,),
        in_specs=[
            by_rows(width_inner),
            by_rows(2 * state_size),
            by_rows(head_count),
            by_rows(width_inner),
            fixed(width_inner),
            pl.BlockSpec((1, width_inner, state_size), lambda b: (b, 0, 0)),
        ],
        out_specs=(by_rows(width_inner), by_rows(1)),
        out_shape=(
            jax.ShapeDtypeStruct((tok_rows, width_inner), jnp.bfloat16),
            jax.ShapeDtypeStruct((tok_rows, 1), jnp.float32),
        ),
        cost_estimate=cost(2 * whole * state_size, 8 * whole, whole),
        name="gate",
    )(intra, bc, cumulative, gate, norm_gain[None, :], jnp.concatenate(states, axis=0))

    square_total = sum_over_tp(squares[:, 0])
    share = tok_rows // size_tp
    mean_square = lax.dynamic_slice(square_total, (me * share,), (share,)) / (width_inner * size_tp)
    scale = lax.rsqrt(mean_square + 1e-05)[:, None]

    if size_tp != 4:
        part = jnp.dot(gated, out_weight, preferred_element_type=jnp.float32).astype(jnp.bfloat16)
        total = lax.psum_scatter(part, "tp", scatter_dimension=0, tiled=True)
        return (total.astype(jnp.float32) * scale).astype(jnp.bfloat16)

    def rows_of(place):
        return lax.dynamic_slice(gated, (place * share, 0), (share, width_inner))

    def reduced(place, weight):
        away = jnp.dot(rows_of(place ^ 1), weight, preferred_element_type=jnp.float32)
        own = jnp.dot(rows_of(place), weight, preferred_element_type=jnp.float32)
        return own + swapped(away.astype(jnp.bfloat16), 1).astype(jnp.float32)

    cuts = 2
    width_out = out_weight.shape[1] // cuts
    results = []
    weights = [out_weight[:, c * width_out : (c + 1) * width_out] for c in range(cuts)]
    arrived = [swapped(reduced(me ^ 2, w).astype(jnp.bfloat16), 2) for w in weights]
    for w, other in zip(weights, arrived):
        total = reduced(me, w) + other.astype(jnp.float32)
        results.append((total * scale).astype(jnp.bfloat16))
    return jnp.concatenate(results, axis=1)


def solution(mesh):
    in_specs = (
        P("seq", "tp"),
        P(None, "tp"),
        P(None, "tp"),
        P(),
        P(None, "tp"),
        P(None, "tp"),
        P(),
        P("tp"),
        P("tp"),
        P("tp"),
        P("tp"),
        P("tp", None),
    )
    out_specs = P(("seq", "tp"), None)
    return jax.shard_map(
        on_device, mesh=mesh, in_specs=in_specs, out_specs=out_specs, check_vma=False
    )
```

```python
import jax
import jax.numpy as jnp
from jax import lax
from jax.experimental import pallas as pl
from jax.experimental.pallas import tpu as pltpu
from jax.sharding import PartitionSpec as P

GROUP = 256
HALO = 16


def swapped(shard, by):
    size = lax.axis_size("tp")
    return lax.ppermute(shard, "tp", [(i, i ^ by) for i in range(size)])


def shifted(shard, by):
    size = lax.axis_size("seq")
    return lax.ppermute(shard, "seq", [(i, i + by) for i in range(size - by)])


def gather_features(rows):
    size = lax.axis_size("tp")
    me = lax.axis_index("tp")
    width = rows.shape[1]
    held = [(0, rows)]
    step = size // 2
    while step >= 1:
        held = held + [(code ^ step, swapped(part, step)) for code, part in held]
        step //= 2
    parts = dict(held)
    full = jnp.zeros((rows.shape[0], width * size), rows.dtype)
    for code in range(size):
        full = lax.dynamic_update_slice(full, parts[code], (0, (me ^ code) * width))
    return full


def sum_over_tp(part):
    size = lax.axis_size("tp")
    step = 1
    while step < size:
        part = part + swapped(part, step)
        step *= 2
    return part


def prefix_kernel(mine_ref, decay_ref, owner_ref, out_ref):
    owner = owner_ref[...]
    carried = jnp.zeros(mine_ref.shape[1:], jnp.float32)
    for i in range(mine_ref.shape[0]):
        out_ref[i] = carried.astype(jnp.bfloat16)
        log_row = jnp.sum(owner * decay_ref[i : i + 1, :], axis=1, keepdims=True)
        carried = carried * jnp.exp(log_row) + mine_ref[i].astype(jnp.float32)


def earlier_state(local_state, decay_total, head_width, cover):
    size = lax.axis_size("seq")
    rows, states = local_state.shape
    share = rows // size
    me = lax.axis_index("seq")
    heads = decay_total.shape[0]
    wide = jnp.pad(decay_total, (0, -heads % 128))
    wide = jnp.broadcast_to(wide[None, None, :], (size, 1, wide.shape[0]))
    decay_all = lax.all_to_all(wide, "seq", 0, 0, tiled=True)[:, 0, :heads]
    blocks = local_state.reshape(size, share, states)
    blocks, decay_all = lax.optimization_barrier((blocks, decay_all))
    mine = lax.all_to_all(blocks, "seq", 0, 0, tiled=True)
    mine, cover = lax.optimization_barrier((mine, cover))
    row_head = (me * share + jnp.arange(share)) // head_width
    owner = (row_head[:, None] == jnp.arange(decay_total.shape[0])[None, :]).astype(jnp.float32)
    prefixes = pl.pallas_call(
        prefix_kernel,
        out_shape=jax.ShapeDtypeStruct(mine.shape, jnp.bfloat16),
        cost_estimate=pl.CostEstimate(flops=0, bytes_accessed=4 * mine.size, transcendentals=0),
    )(mine, decay_all, owner)
    return lax.all_to_all(prefixes, "seq", 0, 0, tiled=True).reshape(rows, states), cover


def per_head(table, first, count, width, lanes):
    lane = lax.broadcasted_iota(jnp.int32, (table.shape[0], lanes), 1)
    spread = jnp.broadcast_to(table[:, first : first + 1], (table.shape[0], lanes))
    for k in range(1, count):
        spread = jnp.where(lane >= k * width, table[:, first + k : first + k + 1], spread)
    return spread


def silu(value):
    return value * (0.5 * jnp.tanh(0.5 * value) + 0.5)


def conv_kernel(blocks, head_width, lanes, *refs):
    inner_refs, state_refs = refs[:blocks], refs[blocks : 2 * blocks]
    tap_inner, tap_state, tail_ref = refs[2 * blocks : 2 * blocks + 3]
    x_ref, bc_ref, contribution_ref = refs[2 * blocks + 3 :]
    taps = tap_inner.shape[0]
    heads_per = lanes // head_width

    def mixed(chunk_refs, b, span, kernel):
        if b == 0:
            padded = chunk_refs[0][:, span].astype(jnp.float32)
        else:
            last = chunk_refs[b - 1].shape[0] - HALO
            edge = chunk_refs[b - 1][last:, span].astype(jnp.float32)
            padded = jnp.concatenate([edge, chunk_refs[b][:, span].astype(jnp.float32)], axis=0)
        total = padded * kernel[taps - 1 : taps]
        for tap in range(taps - 1):
            total = total + pltpu.roll(padded, taps - 1 - tap, 0) * kernel[tap : tap + 1]
        return silu(total[HALO:]).astype(jnp.bfloat16)

    for b in range(blocks):
        rows = slice(b * GROUP, (b + 1) * GROUP)
        bc = mixed(state_refs, b, slice(None), tap_state[...])
        bc_ref[rows] = bc
        inject = bc[:, : bc.shape[1] // 2]
        tail = tail_ref[rows]
        for p in range(x_ref.shape[1] // lanes):
            span = slice(p * lanes, (p + 1) * lanes)
            x = mixed(inner_refs, b, span, tap_inner[:, span])
            x_ref[rows, span] = x
            weight = per_head(tail, p * heads_per, heads_per, head_width, lanes)
            scaled = (x.astype(jnp.float32) * weight).astype(jnp.bfloat16)
            contribution_ref[b, span] = lax.dot_general(
                scaled, inject, (((0,), (0,)), ((), ())), preferred_element_type=jnp.float32
            )


def intra_kernel(head_width, lanes, x_ref, bc_ref, cum_ref, cum_t_ref, step_t_ref, skip_ref, out_ref):
    states = bc_ref.shape[1] // 2
    heads_per = lanes // head_width
    scores = lax.dot_general(
        bc_ref[:, states:], bc_ref[:, :states], (((1,), (1,)), ((), ())),
        preferred_element_type=jnp.float32,
    )
    t = lax.broadcasted_iota(jnp.int32, scores.shape, 0)
    s = lax.broadcasted_iota(jnp.int32, scores.shape, 1)
    scores = jnp.where(s <= t, scores, 0.0)
    lane = lax.broadcasted_iota(jnp.int32, (x_ref.shape[0], lanes), 1)
    for p in range(x_ref.shape[1] // lanes):
        span = slice(p * lanes, (p + 1) * lanes)
        x = x_ref[:, span]
        total = None
        for k in range(heads_per):
            h = p * heads_per + k
            gaps = jnp.minimum(cum_ref[:, h : h + 1] - cum_t_ref[h : h + 1, :], 0.0)
            mixing = (scores * jnp.exp(gaps) * step_t_ref[h : h + 1, :]).astype(jnp.bfloat16)
            part = jnp.dot(mixing, x, preferred_element_type=jnp.float32)
            total = part if k == 0 else jnp.where(lane >= k * head_width, part, total)
        out_ref[:, span] = total + skip_ref[:, span] * x.astype(jnp.float32)


def gate_kernel(head_width, lanes, intra_ref, bc_ref, cum_ref, gate_ref, gain_ref, state_ref, out_ref, square_ref):
    states = bc_ref.shape[1] // 2
    heads_per = lanes // head_width
    readout = bc_ref[:, states:]
    grown = jnp.exp(cum_ref[...])
    squares = jnp.zeros((readout.shape[0], lanes), jnp.float32)
    for p in range(intra_ref.shape[1] // lanes):
        span = slice(p * lanes, (p + 1) * lanes)
        reads = lax.dot_general(
            readout, state_ref[0, span], (((1,), (1,)), ((), ())), preferred_element_type=jnp.float32
        )
        weight = per_head(grown, p * heads_per, heads_per, head_width, lanes)
        g = (intra_ref[:, span] + reads * weight) * silu(gate_ref[:, span].astype(jnp.float32))
        squares = squares + g * g
        out_ref[:, span] = (g * gain_ref[:, span]).astype(jnp.bfloat16)
    square_ref[...] = jnp.sum(squares, axis=1, keepdims=True)


def project(rows, *weights):
    return [jnp.dot(rows, weight, preferred_element_type=jnp.float32) for weight in weights]


def on_device(
    tokens,
    gate_weight,
    inner_weight,
    state_weight,
    step_weight,
    conv_inner,
    conv_state,
    step_bias,
    decay_rate,
    skip_gain,
    norm_gain,
    out_weight,
):
    tok_rows = tokens.shape[0]
    width_inner = inner_weight.shape[1]
    head_count = step_weight.shape[1]
    head_width = width_inner // head_count
    state_size = state_weight.shape[1] // 2
    blocks = tok_rows // GROUP
    size_tp = lax.axis_size("tp")
    me = lax.axis_index("tp")

    chunks = [None] * blocks
    for b in range(blocks - 1, -1, -1):
        chunks[b] = gather_features(tokens[b * GROUP : (b + 1) * GROUP])
    halo = shifted(chunks[-1][GROUP - HALO :], 1)
    chunks[0] = jnp.concatenate([halo, chunks[0]], axis=0)

    inner_raw, state_raw, step_raw = [None] * blocks, [None] * blocks, [None] * blocks
    for b in range(blocks - 1, -1, -1):
        i_b, s_b, t_b = project(chunks[b], inner_weight, state_weight, step_weight)
        inner_raw[b], state_raw[b] = i_b.astype(jnp.bfloat16), s_b.astype(jnp.bfloat16)
        step_raw[b] = t_b[HALO:] if b == 0 else t_b

    lanes = max(128, head_width)
    time_step = jax.nn.softplus(jnp.concatenate(step_raw, axis=0) + step_bias[None, :])
    log_decay = -time_step * decay_rate[None, :]
    grouped = log_decay.reshape(blocks, GROUP, head_count)
    cumulative = jnp.cumsum(grouped, axis=1)
    ending = cumulative[:, -1]
    tail = (jnp.exp(ending[:, None] - cumulative)).reshape(tok_rows, head_count) * time_step
    cumulative = cumulative.reshape(tok_rows, head_count)

    def cost(flops, count, exps):
        return pl.CostEstimate(flops=flops, bytes_accessed=count, transcendentals=exps)

    whole = tok_rows * width_inner
    x, bc, contribution = pl.pallas_call(
        lambda *refs: conv_kernel(blocks, head_width, lanes, *refs),
        out_shape=(
            jax.ShapeDtypeStruct((tok_rows, width_inner), jnp.bfloat16),
            jax.ShapeDtypeStruct((tok_rows, 2 * state_size), jnp.bfloat16),
            jax.ShapeDtypeStruct((blocks, width_inner, state_size), jnp.float32),
        ),
        cost_estimate=cost(2 * whole * state_size, 6 * whole, whole),
        name="conv",
    )(*inner_raw, *state_raw, conv_inner, conv_state, tail)
    contribution = contribution.reshape(blocks, head_count, head_width, state_size)
    local_state = jnp.zeros((head_count, head_width, state_size), jnp.float32)
    for b in range(blocks):
        local_state = jnp.exp(ending[b])[:, None, None] * local_state + contribution[b]

    def by_rows(width):
        return pl.BlockSpec((GROUP, width), lambda b: (b, 0))

    def by_columns(height):
        return pl.BlockSpec((height, GROUP), lambda b: (0, b))

    def fixed(width):
        return pl.BlockSpec((1, width), lambda b: (0, 0))

    intra = pl.pallas_call(
        lambda *refs: intra_kernel(head_width, lanes, *refs),
        grid=(blocks,),
        in_specs=[
            by_rows(width_inner),
            by_rows(2 * state_size),
            by_rows(head_count),
            by_columns(head_count),
            by_columns(head_count),
            fixed(width_inner),
        ],
        out_specs=by_rows(width_inner),
        out_shape=jax.ShapeDtypeStruct((tok_rows, width_inner), jnp.float32),
        cost_estimate=cost(4 * whole * GROUP, 6 * whole, GROUP * tok_rows * head_count),
        name="intra",
    )(x, bc, cumulative, cumulative.T, time_step.T, jnp.repeat(skip_gain, head_width)[None, :])

    gate = jnp.concatenate(
        [
            jnp.dot(c[c.shape[0] - GROUP :], gate_weight, preferred_element_type=jnp.float32).astype(jnp.bfloat16)
            for c in chunks
        ],
        axis=0,
    )

    carried, intra = earlier_state(
        local_state.astype(jnp.bfloat16).reshape(width_inner, state_size),
        jnp.sum(ending, axis=0),
        head_width,
        intra,
    )
    carried = carried.astype(jnp.float32).reshape(head_count, head_width, state_size)
    states = []
    for b in range(blocks):
        states.append(carried.astype(jnp.bfloat16).reshape(1, width_inner, state_size))
        carried = jnp.exp(ending[b])[:, None, None] * carried + contribution[b]

    gated, squares = pl.pallas_call(
        lambda *refs: gate_kernel(head_width, lanes, *refs),
        grid=(blocks,),
        in_specs=[
            by_rows(width_inner),
            by_rows(2 * state_size),
            by_rows(head_count),
            by_rows(width_inner),
            fixed(width_inner),
            pl.BlockSpec((1, width_inner, state_size), lambda b: (b, 0, 0)),
        ],
        out_specs=(by_rows(width_inner), by_rows(1)),
        out_shape=(
            jax.ShapeDtypeStruct((tok_rows, width_inner), jnp.bfloat16),
            jax.ShapeDtypeStruct((tok_rows, 1), jnp.float32),
        ),
        cost_estimate=cost(2 * whole * state_size, 8 * whole, whole),
        name="gate",
    )(intra, bc, cumulative, gate, norm_gain[None, :], jnp.concatenate(states, axis=0))

    square_total = sum_over_tp(squares[:, 0])
    share = tok_rows // size_tp
    mean_square = lax.dynamic_slice(square_total, (me * share,), (share,)) / (width_inner * size_tp)
    scale = lax.rsqrt(mean_square + 1e-05)[:, None]

    if size_tp != 4:
        part = jnp.dot(gated, out_weight, preferred_element_type=jnp.float32).astype(jnp.bfloat16)
        total = lax.psum_scatter(part, "tp", scatter_dimension=0, tiled=True)
        return (total.astype(jnp.float32) * scale).astype(jnp.bfloat16)

    side = me // 2

    def reduced(chip, weight):
        rows = lax.dynamic_slice(gated, (chip * 2 * share, 0), (2 * share, width_inner))
        both = jnp.dot(rows, weight, preferred_element_type=jnp.float32).astype(jnp.bfloat16)
        shape = (share, weight.shape[1])
        away = lax.dynamic_slice(both, ((1 - me % 2) * share, 0), shape)
        own = lax.dynamic_slice(both, ((me % 2) * share, 0), shape)
        return own.astype(jnp.float32) + swapped(away, 1).astype(jnp.float32)

    cuts = 2
    width_out = out_weight.shape[1] // cuts
    weights = [out_weight[:, c * width_out : (c + 1) * width_out] for c in range(cuts)]
    arrived = [swapped(reduced(side ^ 1, w).astype(jnp.bfloat16), 2) for w in weights]
    results = []
    for w, other in zip(weights, arrived):
        total = reduced(side, w) + other.astype(jnp.float32)
        results.append((total * scale).astype(jnp.bfloat16))
    return jnp.concatenate(results, axis=1)


def solution(mesh):
    in_specs = (
        P("seq", "tp"),
        P(None, "tp"),
        P(None, "tp"),
        P(),
        P(None, "tp"),
        P(None, "tp"),
        P(),
        P("tp"),
        P("tp"),
        P("tp"),
        P("tp"),
        P("tp", None),
    )
    out_specs = P(("seq", "tp"), None)
    return jax.shard_map(
        on_device, mesh=mesh, in_specs=in_specs, out_specs=out_specs, check_vma=False
    )
```
